32 devices in a mesh: dp: 8 (over y, x, core), seq: 4 (over z).
Axes of the slice: x: 2, y: 2, z: 4, core: 2. Of those that a mesh axis runs over, the one named last changes fastest.
Arguments:
- tokens_in: bfloat16 [16, 1024, 1536], P('dp', 'seq'), may hold values from -6 to 6
- expert_ids: int32 [16, 1024, 8], P('dp', 'seq'), may hold values from 0 to 15, all different within a row; in each aligned block of 256 rows (0 to 255, 256 to 511, ..., all dimensions but the last counted through in order) at most 160 rows name the same one
- prefix_len: int32 [16], P('dp'), may hold values from 102 to 512
- attn_gain: float32 [1536], P(('dp', 'seq')), may hold values from 0.25 to 1.75
- w_qkv: float32 [1536, 2560], P(('dp', 'seq')), may hold values from -0.625 to 0.625
- w_out: float32 [1536, 1536], P(None, ('dp', 'seq')), may hold values from -0.875 to 0.875
- ffn_gain: float32 [1536], P(('dp', 'seq')), may hold values from 0.25 to 1.75
- w_router: float32 [1536, 16], P(('dp', 'seq')), may hold values from -0.078125 to 0.078125
- w_gate_up: float32 [16, 1536, 1024], P('seq', 'dp'), may hold values from -0.3125 to 0.3125
- w_down: float32 [16, 512, 1536], P('seq', None, 'dp'), may hold values from -1 to 1
- out_grad: bfloat16 [16, 1024, 1536], P('dp', 'seq'), may hold values from -6 to 6
Outputs:
- activations: bfloat16 [16, 1024, 1536], P('dp', 'seq')
- input_grad: float32 [16, 1024, 1536], P('dp', 'seq')
- grad_attn_gain: float32 [1536], P(('dp', 'seq'))
- grad_w_qkv: float32 [1536, 2560], P(('dp', 'seq'))
- grad_w_out: float32 [1536, 1536], P(None, ('dp', 'seq'))
- grad_ffn_gain: float32 [1536], P(('dp', 'seq'))
- grad_w_router: float32 [1536, 16], P(('dp', 'seq'))
- grad_w_gate_up: float32 [16, 1536, 1024], P('seq', 'dp')
- grad_w_down: float32 [16, 512, 1536], P('seq', None, 'dp')
The draws below stay inside these ranges and needn't reach their ends.
Inputs may be any that keep to these rules, and one draw needn't show every extreme that they name: `expert_ids`: within the 256 rows of one sequence on one device (aligned blocks of rows), no expert is named by more than 160 rows, and some block in every draw has an expert named by exactly 160 rows; the 8 experts of a token differ.
All inputs are finite; a program needn't handle non-finite values.
Results may differ from the reference program's by a relative error of at most 0.02.
The reference program's roundings to bfloat16 on the way count: a program that leaves them out, or rounds other values in their place, can miss the bound.
Values may be sent and summed in bfloat16 or wider, within the bound.
A program may use at most 448 MiB of HBM per device.

```python
import math
import jax
import jax.numpy as jnp
import numpy as np
from jax import lax

D = 1536
HEADS = 24
KV = 8
HD = 64
FF = 512
TOP = 8
EXPERTS = 16
SEQ_LEN = 1024
QKV = 2560
SEQS_ALL = 16
SEG = 256
CAP = 160
N_SEQ = 4


def touch_ends(values, stream_key, low, largest):
    extent = values.shape
    index_at = [jax.random.randint(jax.random.fold_in(stream_key, axis), (), 0, extent[axis]) for axis in range(len(extent))]
    values = values.at[tuple(index_at)].set(low)
    longest = extent.index(max(extent))
    index_at[longest] = (index_at[longest] + 1) % extent[longest]
    return values.at[tuple(index_at)].set(largest)


def shard_levels(rng, dims, cuts, smallest, high):
    level = 1.0
    for axis_at, shards_of in cuts:
        draws = jax.random.uniform(jax.random.fold_in(jax.random.fold_in(rng, 6), axis_at), (shards_of,), jnp.float32, smallest / len(cuts), high / len(cuts))
        level = level * jnp.repeat(jnp.exp(draws), dims[axis_at] // shards_of).reshape((-1,) + (1,) * (len(dims) - 1 - axis_at))
    return level


def assign_block(stream_key, own, number, rows, number_of, top, bound, slope):
    ranking = jax.random.permutation(stream_key, number_of)
    heavy_load, ordinary = load_shares(number_of, rows * top, bound, slope, True), load_shares(number_of, rows * top, bound, slope, False)
    places = jnp.arange(number_of)

    def named(lengths, rotation):
        used = int((lengths > 0).sum())
        fixed = max(1, used // 4)
        shifted = fixed + (places - fixed + rotation * (used - fixed)) % max(1, number_of - fixed)
        return jnp.zeros((number_of,), jnp.int32).at[ranking[jnp.where(places < fixed, places, shifted)]].set(jnp.asarray(lengths, jnp.int32))

    lengths = jnp.where(number % 4 == 0, named(heavy_load, number // 4), named(ordinary, number - number // 4 - 1))
    mixed = jax.random.permutation(jax.random.fold_in(own, 3), number_of)
    donor, taker = mixed[0:number_of // 2 * 2:2], mixed[1:number_of // 2 * 2:2]
    room = jnp.minimum(lengths[donor] - 1, bound - lengths[taker]) // 2
    room = jnp.where((donor == ranking[0]) | (taker == ranking[0]) | (lengths[taker] == 0), 0, jnp.maximum(room, 0))
    shifted = jax.random.randint(jax.random.fold_in(own, 4), (number_of // 2,), 0, 1 << 20) % (room + 1)
    lengths = lengths.at[donor].add(-shifted).at[taker].add(shifted)
    items = jnp.searchsorted(jnp.cumsum(lengths), jnp.arange(rows * top), side="right").astype(jnp.int32)
    listing = items.reshape(top, rows).T
    listing = listing[jax.random.permutation(jax.random.fold_in(own, 1), rows)]
    rotation = jax.random.randint(jax.random.fold_in(own, 2), (rows, 1), 0, top)
    return jnp.take_along_axis(listing, (jnp.arange(top)[None, :] + rotation) % top, axis=1)


def load_shares(count, total, limit, lean, full):
    portions = [(1 << 20) // math.isqrt(standing ** lean) + 1 for standing in range(1, count + 1)]
    largest = limit if full else min(limit, max(-(-total // count), total * portions[0] // sum(portions)))
    least = 1 if total - largest >= count - 1 else 0
    given, rest = [largest] + [least] * (count - 1), total - largest - least * (count - 1)
    while rest > 0:
        movable = [i for i in range(1, count) if given[i] < largest] or [i for i in range(1, count) if given[i] < limit]
        mass, budget = sum([portions[i] for i in movable]), rest
        for i in movable:
            extra = min(limit - given[i], max(1, budget * portions[i] // mass), rest)
            given[i] = given[i] + extra
            rest = rest - extra
    return np.array(given)


def gaussian(rng, dims, width, bound, split=(), kind=jnp.bfloat16):
    loudness = shard_levels(rng, dims, split, -0.22, 0.18) if split else 1.0
    drawn = jax.random.normal(rng, dims, jnp.float32) * width * loudness
    return jnp.minimum(jnp.maximum(drawn, -bound), bound).astype(kind)


def setup_inputs(seed: int = 0) -> dict:
    key_of = jax.random.split(jax.random.key(seed), 12)
    tokens_in = gaussian(key_of[0], (SEQS_ALL, SEQ_LEN, D), 1.0, 6.0, ((0, 8), (1, 4)))
    expert_ids_keys = jax.random.split(jax.random.fold_in(key_of[1], 1), SEQS_ALL * SEQ_LEN // SEG)
    expert_ids_turns = jax.random.permutation(jax.random.fold_in(key_of[1], 3), SEQS_ALL * SEQ_LEN // SEG)
    expert_ids = jax.vmap(lambda own, number: assign_block(jax.random.fold_in(key_of[1], 2), own, number, SEG, EXPERTS, TOP, CAP, 2))(expert_ids_keys, expert_ids_turns).reshape((SEQS_ALL, SEQ_LEN, TOP))
    prefix_len = touch_ends(jax.random.randint(key_of[2], (SEQS_ALL,), SEQ_LEN // 10, SEQ_LEN // 2 + 1), jax.random.fold_in(key_of[2], 1), SEQ_LEN // 10, (SEQ_LEN // 2 + 1) - 1).astype(jnp.int32)
    attn_gain = jnp.clip(1.0 + 0.15 * jax.random.normal(key_of[3], (D,), jnp.float32), 0.25, 1.75)
    w_qkv = gaussian(key_of[4], (D, QKV), (D // 16) ** -0.5, 0.625, ((0, 32),), jnp.float32)
    w_out = gaussian(key_of[5], (HEADS * HD, D), (HEADS * HD // 32) ** -0.5, 0.875, ((1, 32),), jnp.float32)
    ffn_gain = jnp.clip(1.0 + 0.15 * jax.random.normal(key_of[6], (D,), jnp.float32), 0.25, 1.75)
    w_router = gaussian(key_of[7], (D, EXPERTS), (4 * D) ** -0.5, 0.078125, ((0, 32),), jnp.float32)
    w_gate_up = gaussian(key_of[8], (EXPERTS, D, 2 * FF), (D // 4) ** -0.5, 0.3125, ((0, 4), (1, 8)), jnp.float32)
    w_down = gaussian(key_of[9], (EXPERTS, FF, D), (FF // 16) ** -0.5, 1.0, ((0, 4), (2, 8)), jnp.float32)
    out_grad = gaussian(key_of[10], (SEQS_ALL, SEQ_LEN, D), 1.0, 6.0, ((0, 8), (1, 4)))
    return {"tokens_in": tokens_in, "expert_ids": expert_ids, "prefix_len": prefix_len, "attn_gain": attn_gain, "w_qkv": w_qkv, "w_out": w_out, "ffn_gain": ffn_gain, "w_router": w_router, "w_gate_up": w_gate_up, "w_down": w_down, "out_grad": out_grad}


EPSILON = 1e-06
SCORE_SCALE = 0.015625
RESIDUAL_FACTOR = 0.22
ROTARY_BASE = 10000.0
NEGATIVE_FILL = -1e+30
TOP_PRECISION = lax.Precision.HIGHEST

@jax.custom_vjp
def low(v):
    return lax.optimization_barrier(v.astype(jnp.bfloat16)).astype(jnp.float32)

@jax.custom_vjp
def reduced_precision_backward(v):
    return v

def low_keep(v):
    return (low(v), None)

def low_pass(kept, grad):
    return (grad,)

def back_keep(v):
    return (v, None)

def back_low(kept, grad):
    return (low(grad),)
low.defvjp(low_keep, low_pass)
reduced_precision_backward.defvjp(back_keep, back_low)

def rotary_tables(positions):
    half_size = HD // 2
    inverse = ROTARY_BASE ** (-(jnp.arange(half_size, dtype=jnp.float32) * 2.0 / HD))
    angles = positions.astype(jnp.float32)[:, None] * inverse[None, :]
    return (jnp.cos(angles)[:, None, :], jnp.sin(angles)[:, None, :])

def rotate(values, cosine_table, sine_table, direction):
    half_size = values.shape[-1] // 2
    first_half = values[..., :half_size]
    second_half = values[..., half_size:]
    return jnp.concatenate([first_half * cosine_table - direction * second_half * sine_table, second_half * cosine_table + direction * first_half * sine_table], axis=-1)

def root_norm(values, gain_row):
    scale_row = lax.rsqrt(lax.optimization_barrier(jnp.mean(values * values, axis=-1, keepdims=True)) + EPSILON)
    return values * scale_row * gain_row

def visible(query_pos, key_pos, prefix):
    return (key_pos[None, :] <= query_pos[:, None]) | (key_pos[None, :] < prefix) & (query_pos[:, None] < prefix)

def expert_slots(routed, capacity):
    one_hot = (routed[..., None] == jnp.arange(EXPERTS, dtype=jnp.int32)).astype(jnp.int32)
    before = jnp.cumsum(one_hot, axis=1) - one_hot
    return (routed * capacity + lax.optimization_barrier(jnp.sum(before * one_hot, axis=-1))).astype(jnp.int32)

def attend_rows(queries, keys_seq, values_seq, row_start, prefix):
    block_rows = queries.shape[0]
    query_pos = row_start + jnp.arange(block_rows, dtype=jnp.int32)
    key_pos = jnp.arange(SEQ_LEN, dtype=jnp.int32)
    scores = jnp.einsum('qhgd,khd->hgqk', queries, keys_seq, precision=TOP_PRECISION)
    scores = jnp.where(visible(query_pos, key_pos, prefix)[None, None], reduced_precision_backward(SCORE_SCALE * scores), NEGATIVE_FILL)
    row_max = lax.optimization_barrier(jnp.max(scores, axis=-1, keepdims=True))
    exp_weights = jnp.exp(scores - row_max)
    sum_exp = lax.optimization_barrier(jnp.sum(exp_weights, axis=-1))
    mixed_sum = reduced_precision_backward(jnp.einsum('hgqk,khd->qhgd', low(exp_weights), values_seq, precision=TOP_PRECISION))
    return low(mixed_sum / jnp.transpose(sum_exp, (2, 0, 1))[..., None])

def block_layer(token_batch, weight_set, routes, prefixes):
    gain_attn, query_key_value_matrix, output_matrix, gain_ffn, routing_matrix, gate_up_weight, down_weight = [low(weight) for weight in weight_set]
    seq_count = token_batch.shape[0]
    query_group = HEADS // KV
    attention_input_normed = low(root_norm(token_batch, gain_attn))
    output_projection = reduced_precision_backward(jnp.einsum('rcp,pa->rca', attention_input_normed, query_key_value_matrix, precision=TOP_PRECISION))
    cosine_table, sine_table = rotary_tables(jnp.arange(SEQ_LEN, dtype=jnp.int32))
    queries = low(rotate(output_projection[..., :HEADS * HD].reshape(seq_count, SEQ_LEN, HEADS, HD), cosine_table, sine_table, 1.0))
    keys_all = low(rotate(output_projection[..., HEADS * HD:(HEADS + KV) * HD].reshape(seq_count, SEQ_LEN, KV, HD), cosine_table, sine_table, 1.0))
    values_all = low(output_projection[..., (HEADS + KV) * HD:].reshape(seq_count, SEQ_LEN, KV, HD))
    block_rows = min(512, SEQ_LEN)
    block_count = SEQ_LEN // block_rows

    def one_sequence(seq_items):
        seq_queries, seq_keys, seq_values, prefix = seq_items
        blocks = seq_queries.reshape(block_count, block_rows, KV, query_group, HD)
        starts = jnp.arange(block_count, dtype=jnp.int32) * block_rows

        def one_block(block_pair):
            return attend_rows(block_pair[0], seq_keys, seq_values, block_pair[1], prefix)
        return lax.map(jax.checkpoint(one_block), (blocks, starts)).reshape(SEQ_LEN, HEADS * HD)
    attention_result = lax.map(one_sequence, (queries, keys_all, values_all, prefixes))
    initial_residual_sum = token_batch + RESIDUAL_FACTOR * reduced_precision_backward(jnp.einsum('rtm,mg->rtg', attention_result, output_matrix, precision=TOP_PRECISION))
    feedforward_input_normed = low(root_norm(initial_residual_sum, gain_ffn))
    router_scores = reduced_precision_backward(jnp.einsum('rcp,pa->rca', feedforward_input_normed, routing_matrix, precision=TOP_PRECISION))
    one_hot = (routes[..., None] == jnp.arange(EXPERTS, dtype=jnp.int32)).astype(jnp.float32)
    chosen = lax.optimization_barrier(jnp.sum(one_hot * router_scores[:, :, None, :], axis=-1))
    gate_weights = jax.nn.softmax(chosen, axis=-1)
    segments = seq_count * N_SEQ
    seg_rows = feedforward_input_normed.reshape(segments, SEG, D)
    slot_index = expert_slots(routes.reshape(segments, SEG * TOP), CAP)
    token_of = jnp.arange(SEG * TOP, dtype=jnp.int32) // TOP

    def place_rows(row_block, slot_row):
        return jnp.zeros((EXPERTS * CAP, D), jnp.float32).at[slot_row].set(row_block[token_of])
    buffers = jax.vmap(place_rows)(seg_rows, slot_index).reshape(segments, EXPERTS, CAP, D)
    gate_up = reduced_precision_backward(jnp.einsum('secd,edf->secf', buffers, gate_up_weight, precision=TOP_PRECISION))
    activated = low(jax.nn.silu(gate_up[..., :FF]) * gate_up[..., FF:])
    expert_out = low(reduced_precision_backward(jnp.einsum('secf,efd->secd', activated, down_weight, precision=TOP_PRECISION)))
    flat_out = expert_out.reshape(segments, EXPERTS * CAP, D)
    picked = jax.vmap(lambda row_block, slot_row: row_block[slot_row])(flat_out, slot_index)
    picked = picked.reshape(seq_count, SEQ_LEN, TOP, D)
    return initial_residual_sum + RESIDUAL_FACTOR * lax.optimization_barrier(jnp.sum(gate_weights[..., None] * picked, axis=2))

def reference(tokens_in, expert_ids, prefix_len, attn_gain, w_qkv, w_out, ffn_gain, w_router, w_gate_up, w_down, out_grad):
    weight_set = (attn_gain, w_qkv, w_out, ffn_gain, w_router, w_gate_up, w_down)
    together = math.gcd(SEQS_ALL, max(1, 4096 // SEQ_LEN))
    rounds = SEQS_ALL // together
    inputs = tokens_in.astype(jnp.float32).reshape(rounds, together, SEQ_LEN, D)
    cotangents = out_grad.astype(jnp.float32).reshape(rounds, together, SEQ_LEN, D)
    routed = expert_ids.reshape(rounds, together, SEQ_LEN, TOP)
    prefixes = prefix_len.reshape(rounds, together)

    def one_round(grad_sums, round_items):
        token_batch, routes, prefix_rows, cotangent = round_items
        result, pull_back = jax.vjp(lambda token_rows, weights_now: block_layer(token_rows, weights_now, routes, prefix_rows), token_batch, weight_set)
        token_grad, weight_grads = pull_back(cotangent)
        grad_sums = jax.tree.map(lambda former, latter: former + latter, grad_sums, weight_grads)
        return (grad_sums, (result.astype(jnp.bfloat16), token_grad))
    start_sums = tuple((jnp.zeros_like(weight) for weight in weight_set))
    grad_sums, (results, token_grads) = lax.scan(one_round, start_sums, (inputs, routed, prefixes, cotangents))
    return (results.reshape(SEQS_ALL, SEQ_LEN, D), token_grads.reshape(SEQS_ALL, SEQ_LEN, D), grad_sums[0], grad_sums[1], grad_sums[2], grad_sums[3], grad_sums[4], grad_sums[5], grad_sums[6])
```

```python
import functools

import jax
import jax.numpy as jnp
from jax import lax
from jax.experimental import pallas as pl
from jax.experimental.pallas import tpu as pltpu
from jax.sharding import PartitionSpec as P

HEADS = 24
KV = 8
HD = 64
EXPERTS = 16
EPSILON = 1e-06
SCORE_SCALE = 0.015625
RESIDUAL_FACTOR = 0.22
ROTARY_BASE = 10000.0
NEGATIVE_FILL = -1e30
BF = jnp.bfloat16
F32 = jnp.float32
LANES = 128
GROUP = HEADS // KV
PAIR_Q = 2 * GROUP * HD
VMEM_LIMIT = 62 * 1024 * 1024


def nt(a, b):
    return lax.dot_general(a, b, (((1,), (1,)), ((), ())), preferred_element_type=F32)


def nn(a, b):
    return lax.dot_general(a, b, (((1,), (0,)), ((), ())), preferred_element_type=F32)


def tn(a, b):
    return lax.dot_general(a, b, (((0,), (0,)), ((), ())), preferred_element_type=F32)


def rotary_tables(seg_len):
    half = HD // 2
    positions = lax.axis_index("seq") * seg_len + jnp.arange(seg_len, dtype=jnp.int32)
    inverse = ROTARY_BASE ** (-(jnp.arange(half, dtype=F32) * 2.0 / HD))
    angles = positions.astype(F32)[:, None] * inverse[None, :]
    cosine = jnp.tile(jnp.cos(angles), (1, LANES // half))
    sine = jnp.sin(angles)
    sine = jnp.concatenate([-sine, sine] * (LANES // HD), axis=1)
    return cosine, sine


def rotate_lanes(values, cosine, sine):
    lane = lax.broadcasted_iota(jnp.int32, values.shape, 1)
    half = HD // 2
    swapped = jnp.where(
        lane % HD < half, pltpu.roll(values, LANES - half, 1), pltpu.roll(values, half, 1)
    )
    return values * cosine + swapped * sine


def rope_kernel(x_ref, cos_ref, sin_ref, q_ref, kv_ref):
    cosine, sine = cos_ref[...], sin_ref[...]
    q_cols, kv_cols = HEADS * HD, KV * HD
    for c in range(q_cols // LANES):
        cols = pl.ds(c * LANES, LANES)
        q_ref[0, :, cols] = rotate_lanes(x_ref[0, :, cols], cosine, sine).astype(BF)
    for c in range(kv_cols // LANES):
        cols = pl.ds(c * LANES, LANES)
        source = x_ref[0, :, pl.ds(q_cols + c * LANES, LANES)]
        kv_ref[0, 0, :, cols] = rotate_lanes(source, cosine, sine).astype(BF)
        kv_ref[1, 0, :, cols] = x_ref[0, :, pl.ds(q_cols + kv_cols + c * LANES, LANES)].astype(BF)


def rope(qkv, cosine, sine):
    seqs, seg_len, width = qkv.shape
    return pl.pallas_call(
        rope_kernel,
        grid=(seqs,),
        in_specs=[
            pl.BlockSpec((1, seg_len, width), lambda s: (s, 0, 0)),
            pl.BlockSpec((seg_len, LANES), lambda s: (0, 0)),
            pl.BlockSpec((seg_len, LANES), lambda s: (0, 0)),
        ],
        out_specs=[
            pl.BlockSpec((1, seg_len, HEADS * HD), lambda s: (s, 0, 0)),
            pl.BlockSpec((2, 1, seg_len, KV * HD), lambda s: (0, s, 0, 0)),
        ],
        out_shape=[
            jax.ShapeDtypeStruct((seqs, seg_len, HEADS * HD), BF),
            jax.ShapeDtypeStruct((2, seqs, seg_len, KV * HD), BF),
        ],
        name="rope",
    )(qkv, cosine, sine)


def unrope_kernel(dq_ref, dkv_ref, cos_ref, sin_ref, out_ref):
    cosine, sine = cos_ref[...], -sin_ref[...]
    q_cols, kv_cols = HEADS * HD, KV * HD
    for c in range(q_cols // LANES):
        cols = pl.ds(c * LANES, LANES)
        out_ref[0, :, cols] = rotate_lanes(dq_ref[0, :, cols], cosine, sine).astype(BF)
    for c in range(kv_cols // LANES):
        cols = pl.ds(c * LANES, LANES)
        keys = dkv_ref[0, 0, :, cols].astype(F32)
        out_ref[0, :, pl.ds(q_cols + c * LANES, LANES)] = rotate_lanes(keys, cosine, sine).astype(BF)
        out_ref[0, :, pl.ds(q_cols + kv_cols + c * LANES, LANES)] = dkv_ref[1, 0, :, cols].astype(BF)


def unrope(dq, dkv, cosine, sine):
    seqs, seg_len, q_cols = dq.shape
    kv_cols = KV * HD
    width = q_cols + 2 * kv_cols
    return pl.pallas_call(
        unrope_kernel,
        grid=(seqs,),
        in_specs=[
            pl.BlockSpec((1, seg_len, q_cols), lambda s: (s, 0, 0)),
            pl.BlockSpec((2, 1, seg_len, kv_cols), lambda s: (0, s, 0, 0)),
            pl.BlockSpec((seg_len, LANES), lambda s: (0, 0)),
            pl.BlockSpec((seg_len, LANES), lambda s: (0, 0)),
        ],
        out_specs=pl.BlockSpec((1, seg_len, width), lambda s: (s, 0, 0)),
        out_shape=jax.ShapeDtypeStruct((seqs, seg_len, width), BF),
        name="unrope",
    )(dq, dkv, cosine, sine)


def spread_heads(source, scratch, rows, scale=None):
    lane = lax.broadcasted_iota(jnp.int32, (rows, LANES), 1)
    for head in range(2 * GROUP):
        odd = head >= GROUP
        group, high = divmod(head, 2)
        values = source(group)
        if bool(high) != odd:
            values = pltpu.roll(values, HD, 1)
        keep = lane >= HD if odd else lane < HD
        values = jnp.where(keep, values, jnp.zeros_like(values))
        if scale is not None:
            values = values * scale
        scratch[pl.ds(head * rows, rows), :] = values.astype(scratch.dtype)


def gather_heads(scratch, rows, sink):
    lane = lax.broadcasted_iota(jnp.int32, (rows, LANES), 1)
    for group in range(GROUP):
        parts = []
        for high in range(2):
            head = 2 * group + high
            odd = head >= GROUP
            values = scratch[pl.ds(head * rows, rows), :]
            if bool(high) != odd:
                values = pltpu.roll(values, HD, 1)
            parts.append(values)
        sink(group, jnp.where(lane < HD, parts[0], parts[1]))


def query_limits(info_ref, rows, seqs):
    prefix = info_ref[pl.program_id(0)]
    start = info_ref[seqs] * rows
    position = start + lax.broadcasted_iota(jnp.int32, (rows, 1), 0)
    return jnp.where(position < prefix, prefix, position + 1)


def attention_kernel(seqs, info_ref, q_ref, k_ref, v_ref, o_ref, ml_ref, q_all, o_all):
    rows = q_ref.shape[1]
    keys = k_ref.shape[0] * k_ref.shape[3]
    limit = query_limits(info_ref, rows, seqs)
    spread_heads(lambda g: q_ref[0, :, pl.ds(g * LANES, LANES)].astype(F32), q_all, rows, SCORE_SCALE)
    lane = lax.broadcasted_iota(jnp.int32, (rows, LANES), 1)

    def one_head(head, ml):
        q = q_all[pl.ds(pl.multiple_of(head * rows, rows), rows), :]
        k = k_ref[:, 0, 0].reshape(keys, LANES)
        v = v_ref[:, 0, 0].reshape(keys, LANES)
        scores = nt(q, k)
        position = lax.broadcasted_iota(jnp.int32, (rows, keys), 1)
        scores = jnp.where(position < limit, scores, NEGATIVE_FILL)
        top = jnp.max(scores, axis=1, keepdims=True)
        weights = jnp.exp(scores - top)
        total = jnp.sum(weights, axis=1, keepdims=True)
        mixed = nn(weights.astype(BF), v)
        o_all[pl.ds(pl.multiple_of(head * rows, rows), rows), :] = mixed / total
        ml = jnp.where(lane == head, top, ml)
        return jnp.where(lane == head + HD, total, ml)

    ml_ref[0, 0] = lax.fori_loop(0, 2 * GROUP, one_head, jnp.zeros((rows, LANES), F32))

    def sink(group, values):
        o_ref[0, :, pl.ds(group * LANES, LANES)] = values.astype(BF)

    gather_heads(o_all, rows, sink)


def kv_specs(pieces, seg_len):
    return [
        pl.BlockSpec((pieces, 1, 1, seg_len, LANES), lambda s, p, info: (0, 0, s, 0, p)),
        pl.BlockSpec((pieces, 1, 1, seg_len, LANES), lambda s, p, info: (0, 1, s, 0, p)),
    ]


def attention(info, queries, kv_all):
    seqs, seg_len, width = queries.shape
    pieces = kv_all.shape[0]
    head_rows = 2 * GROUP * seg_len
    pairs = KV // 2
    return pl.pallas_call(
        functools.partial(attention_kernel, seqs),
        grid_spec=pltpu.PrefetchScalarGridSpec(
            num_scalar_prefetch=1,
            grid=(seqs, pairs),
            in_specs=[pl.BlockSpec((1, seg_len, PAIR_Q), lambda s, p, info: (s, 0, p))]
            + kv_specs(pieces, seg_len),
            out_specs=[
                pl.BlockSpec((1, seg_len, PAIR_Q), lambda s, p, info: (s, 0, p)),
                pl.BlockSpec((1, 1, seg_len, LANES), lambda s, p, info: (s, p, 0, 0)),
            ],
            scratch_shapes=[
                pltpu.VMEM((head_rows, LANES), BF),
                pltpu.VMEM((head_rows, LANES), F32),
            ],
        ),
        out_shape=[
            jax.ShapeDtypeStruct((seqs, seg_len, width), BF),
            jax.ShapeDtypeStruct((seqs, pairs, seg_len, LANES), F32),
        ],
        compiler_params=pltpu.CompilerParams(vmem_limit_bytes=VMEM_LIMIT),
        name="attention",
    )(info, queries, kv_all, kv_all)


def attention_back_kernel(
    seqs, info_ref, q_ref, k_ref, v_ref, o_ref, g_ref, ml_ref, dq_ref, dkv_ref,
    q_all, o_all, g_all, dq_all, dk_all, dv_all,
):
    rows = q_ref.shape[1]
    pieces, seg_len = k_ref.shape[0], k_ref.shape[3]
    keys = pieces * seg_len
    limit = query_limits(info_ref, rows, seqs)

    def columns(ref):
        return lambda g: ref[0, :, pl.ds(g * LANES, LANES)].astype(F32)

    spread_heads(columns(q_ref), q_all, rows, SCORE_SCALE)
    spread_heads(columns(o_ref), o_all, rows)
    spread_heads(columns(g_ref), g_all, rows)
    lane = lax.broadcasted_iota(jnp.int32, (rows, LANES), 1)
    dk_all[...] = jnp.zeros_like(dk_all)
    dv_all[...] = jnp.zeros_like(dv_all)
    ml = ml_ref[0, 0]

    def one_head(head, carry):
        part = pl.ds(pl.multiple_of(head * rows, rows), rows)
        q = q_all[part, :]
        k = k_ref[:, 0, 0].reshape(keys, LANES)
        v = v_ref[:, 0, 0].reshape(keys, LANES)
        top = jnp.sum(jnp.where(lane == head, ml, 0.0), axis=1, keepdims=True)
        total = jnp.sum(jnp.where(lane == head + HD, ml, 0.0), axis=1, keepdims=True)
        grad = g_all[part, :]
        grad_total = -jnp.sum(grad * o_all[part, :], axis=1, keepdims=True) / total
        grad_mix = (grad / total).astype(BF)
        scores = nt(q, k)
        position = lax.broadcasted_iota(jnp.int32, (rows, keys), 1)
        scores = jnp.where(position < limit, scores, NEGATIVE_FILL)
        weights = jnp.exp(scores - top)
        grad_weights = nt(grad_mix, v) + grad_total
        grad_scores = (weights * grad_weights).astype(BF)
        dq_all[part, :] = nn(grad_scores, k) * SCORE_SCALE
        dk_all[...] += tn(grad_scores, q)
        dv_all[...] += tn(weights.astype(BF), grad_mix)
        return carry

    lax.fori_loop(0, 2 * GROUP, one_head, 0)

    def sink(group, values):
        dq_ref[0, :, pl.ds(group * LANES, LANES)] = values

    gather_heads(dq_all, rows, sink)
    dkv_ref[:, 0, 0] = dk_all[...].astype(BF).reshape(pieces, seg_len, LANES)
    dkv_ref[:, 1, 0] = dv_all[...].astype(BF).reshape(pieces, seg_len, LANES)


def attention_back(info, queries, kv_all, attended, grads, ml):
    seqs, seg_len, width = queries.shape
    pieces = kv_all.shape[0]
    head_rows = 2 * GROUP * seg_len
    pairs = KV // 2
    rows_spec = pl.BlockSpec((1, seg_len, PAIR_Q), lambda s, p, info: (s, 0, p))
    return pl.pallas_call(
        functools.partial(attention_back_kernel, seqs),
        grid_spec=pltpu.PrefetchScalarGridSpec(
            num_scalar_prefetch=1,
            grid=(seqs, pairs),
            in_specs=[rows_spec]
            + kv_specs(pieces, seg_len)
            + [
                rows_spec,
                rows_spec,
                pl.BlockSpec((1, 1, seg_len, LANES), lambda s, p, info: (s, p, 0, 0)),
            ],
            out_specs=[
                rows_spec,
                pl.BlockSpec((pieces, 2, 1, seg_len, LANES), lambda s, p, info: (0, 0, s, 0, p)),
            ],
            scratch_shapes=[
                pltpu.VMEM((head_rows, LANES), BF),
                pltpu.VMEM((head_rows, LANES), F32),
                pltpu.VMEM((head_rows, LANES), F32),
                pltpu.VMEM((head_rows, LANES), F32),
                pltpu.VMEM((pieces * seg_len, LANES), F32),
                pltpu.VMEM((pieces * seg_len, LANES), F32),
            ],
        ),
        out_shape=[
            jax.ShapeDtypeStruct((seqs, seg_len, width), F32),
            jax.ShapeDtypeStruct((pieces, 2, seqs, seg_len, KV * HD), BF),
        ],
        compiler_params=pltpu.CompilerParams(vmem_limit_bytes=VMEM_LIMIT),
        name="attention_back",
    )(info, queries, kv_all, kv_all, attended, grads, ml)


def experts_kernel(
    h_ref, ht_ref, go_ref, got_ref, gate_ref, w_ref,
    out_ref, dh_ref, dgate_ref, gw_ref,
    out_acc, dh_acc, act_all, dgu_all,
):
    expert = pl.program_id(0)
    tokens, width = h_ref.shape
    slots, slice_len = w_ref.shape[0], w_ref.shape[2]
    hidden = act_all.shape[1]
    rows = min(512, tokens)
    wide = 768
    wide_slots = wide // slice_len

    @pl.when(expert == 0)
    def _():
        out_acc[...] = jnp.zeros_like(out_acc)
        dh_acc[...] = jnp.zeros_like(dh_acc)
        dgate_ref[...] = jnp.zeros_like(dgate_ref)

    def weight(cols):
        return w_ref[:, 0, :, cols].reshape(width, cols.size)

    def token_block(block, carry):
        part = pl.ds(pl.multiple_of(block * rows, rows), rows)
        lane = lax.broadcasted_iota(jnp.int32, (rows, LANES), 1)
        gate = jnp.sum(jnp.where(lane == expert, gate_ref[part, :], 0.0), axis=1, keepdims=True)
        h = h_ref[part, :]
        g = nn(h, weight(pl.ds(0, hidden)))
        up = nn(h, weight(pl.ds(hidden, hidden)))
        da = nn(go_ref[part, :], weight(pl.ds(2 * hidden, hidden))) * RESIDUAL_FACTOR
        sig = 1.0 / (1.0 + jnp.exp(-g))
        silu = g * sig
        act = silu * up
        act_all[part, :] = (gate * act).astype(BF)
        dgate = jnp.sum(act * da, axis=1, keepdims=True)
        dgate_ref[part, :] = jnp.where(lane == expert, dgate, dgate_ref[part, :])
        dact = gate * da
        dgu_all[part, pl.ds(0, hidden)] = (dact * up * (sig * (1.0 + g * (1.0 - sig)))).astype(BF)
        dgu_all[part, pl.ds(hidden, hidden)] = (dact * silu).astype(BF)
        for n in range(width // wide):
            some = pl.ds(n * wide_slots, wide_slots)
            cols = pl.ds(n * wide, wide)
            down = w_ref[some, 0, :, pl.ds(2 * hidden, hidden)].reshape(wide, hidden)
            out_acc[part, cols] += nt(act_all[part, :], down)
            gate_up = w_ref[some, 0, :, pl.ds(0, 2 * hidden)].reshape(wide, 2 * hidden)
            dh_acc[part, cols] += nt(dgu_all[part, :], gate_up)
        return carry

    lax.fori_loop(0, tokens // rows, token_block, 0)

    tall = 384
    tall_slots = tall // slice_len

    def weight_block(block, carry):
        part = pl.ds(pl.multiple_of(block * tall, tall), tall)
        some = pl.ds(block * tall_slots, tall_slots)
        gw_gate_up = nn(ht_ref[part, :], dgu_all[...]).astype(BF)
        gw_ref[some, 0, :, pl.ds(0, 2 * hidden)] = gw_gate_up.reshape(
            tall_slots, slice_len, 2 * hidden
        )
        gw_down = (nn(got_ref[part, :], act_all[...]) * RESIDUAL_FACTOR).astype(BF)
        gw_ref[some, 0, :, pl.ds(2 * hidden, hidden)] = gw_down.reshape(
            tall_slots, slice_len, hidden
        )
        return carry

    lax.fori_loop(0, width // tall, weight_block, 0)

    @pl.when(expert == pl.num_programs(0) - 1)
    def _():
        out_ref[...] = out_acc[...].astype(BF)
        dh_ref[...] = dh_acc[...].astype(BF)


def experts_pass(h, ht, go, got, gates, weights):
    tokens, width = h.shape
    slots, experts, slice_len, packed = weights.shape
    hidden = packed // 3
    one = pl.Buffered(1)
    fixed = lambda shape: pl.BlockSpec(shape, lambda e: (0, 0), pipeline_mode=one)
    moving = pl.BlockSpec((slots, 1, slice_len, packed), lambda e: (0, e, 0, 0))
    flops = 2 * 9 * tokens * width * hidden * experts
    return pl.pallas_call(
        experts_kernel,
        grid=(experts,),
        in_specs=[
            fixed((tokens, width)),
            fixed((width, tokens)),
            fixed((tokens, width)),
            fixed((width, tokens)),
            fixed((tokens, LANES)),
            moving,
        ],
        out_specs=[
            fixed((tokens, width)),
            fixed((tokens, width)),
            fixed((tokens, LANES)),
            moving,
        ],
        out_shape=[
            jax.ShapeDtypeStruct((tokens, width), BF),
            jax.ShapeDtypeStruct((tokens, width), BF),
            jax.ShapeDtypeStruct((tokens, LANES), F32),
            jax.ShapeDtypeStruct(weights.shape, BF),
        ],
        scratch_shapes=[
            pltpu.VMEM((tokens, width), F32),
            pltpu.VMEM((tokens, width), F32),
            pltpu.VMEM((tokens, hidden), BF),
            pltpu.VMEM((tokens, 2 * hidden), BF),
        ],
        compiler_params=pltpu.CompilerParams(vmem_limit_bytes=VMEM_LIMIT),
        cost_estimate=pl.CostEstimate(
            flops=flops, transcendentals=tokens * hidden * experts, bytes_accessed=4 * weights.size
        ),
        name="experts",
    )(h, ht, go, got, gates, weights)


def norm_back(grad_norm, normed, scale_row):
    return scale_row * (grad_norm - normed * jnp.mean(grad_norm * normed, axis=-1, keepdims=True))


def body(
    tokens_in, expert_ids, prefix_len, attn_gain, w_qkv, w_out, ffn_gain, w_router,
    w_gate_up, w_down, out_grad,
):
    seqs, seg_len, width = tokens_in.shape
    tokens = seqs * seg_len
    n_dp, n_seq = lax.axis_size("dp"), lax.axis_size("seq")
    everyone = ("dp", "seq")
    rounds = n_seq // 2
    held = w_gate_up.shape[0]
    me = lax.axis_index("seq")

    def swap(values, bit):
        return lax.ppermute(values, "seq", [(i, i ^ bit) for i in range(n_seq)])

    gains = lax.all_gather(jnp.stack([attn_gain, ffn_gain]).astype(BF), everyone, axis=1, tiled=True)
    gain_attn, gain_ffn = gains[0].astype(F32), gains[1].astype(F32)
    qkv_matrix = lax.all_gather(w_qkv.astype(BF), everyone, axis=0, tiled=True)
    packed = jnp.concatenate([w_gate_up.astype(BF), jnp.swapaxes(w_down, 1, 2).astype(BF)], axis=2)
    packed_rounds = [packed] + [swap(packed, 2 * r) for r in range(1, rounds)]
    out_matrix = lax.all_gather(w_out.T.astype(BF), everyone, axis=0, tiled=True)
    router_matrix = lax.all_gather(w_router.astype(BF), everyone, axis=0, tiled=True)
    expert_rounds = [lax.all_gather(p, "dp", axis=0) for p in packed_rounds]

    go_mine = out_grad.reshape(tokens, width)
    go = jnp.concatenate([go_mine, swap(go_mine, 1)], axis=0)
    ids_mine = expert_ids.reshape(tokens, -1)
    ids = jnp.concatenate([ids_mine, swap(ids_mine, 1)], axis=0)
    got = go.T

    x = tokens_in.reshape(tokens, width).astype(F32)
    scale_one = lax.rsqrt(jnp.mean(x * x, axis=-1, keepdims=True) + EPSILON)
    normed_one = x * scale_one
    h1 = (normed_one * gain_attn).astype(BF)
    qkv = nn(h1, qkv_matrix)
    cosine, sine = rotary_tables(seg_len)
    queries, kv_mine = rope(qkv.reshape(seqs, seg_len, -1), cosine, sine)
    kv_all = lax.all_gather(kv_mine, "seq", axis=0)
    info = jnp.concatenate([prefix_len, me[None].astype(jnp.int32)])
    attended, ml = attention(info, queries, kv_all)
    att = attended.reshape(tokens, width)
    r1 = x + RESIDUAL_FACTOR * nt(att, out_matrix)
    scale_two = lax.rsqrt(jnp.mean(r1 * r1, axis=-1, keepdims=True) + EPSILON)
    normed_two = r1 * scale_two
    h2_mine = (normed_two * gain_ffn).astype(BF)

    h2 = jnp.concatenate([h2_mine, swap(h2_mine, 1)], axis=0)
    h2t = h2.T
    logits = nn(h2, router_matrix)
    routed = jnp.any(ids[:, :, None] == jnp.arange(EXPERTS, dtype=jnp.int32), axis=1)
    chosen = jnp.where(routed, logits, NEGATIVE_FILL)
    chosen = jnp.exp(chosen - jnp.max(chosen, axis=-1, keepdims=True))
    chosen = jnp.where(routed, chosen, 0.0)
    gates = chosen / jnp.sum(chosen, axis=-1, keepdims=True)

    out_part = 0.0
    dh_part = 0.0
    dgates = jnp.zeros((tokens, EXPERTS), F32)
    dgates_away = []
    weight_grads = []
    for r in range(rounds):
        local = lax.dynamic_slice_in_dim(gates, (me ^ (2 * r)) * held, held, 1)
        local = jnp.pad(local, ((0, 0), (0, LANES - held)))
        out_r, dh_r, dgate_r, gw_r = experts_pass(h2, h2t, go, got, local, expert_rounds[r])
        out_part = out_part + out_r.astype(F32)
        dh_part = dh_part + dh_r.astype(F32)
        dgates = lax.dynamic_update_slice_in_dim(
            dgates, dgate_r[:tokens, :held], (me ^ (2 * r)) * held, 1
        )
        dgates_away.append(dgate_r[tokens:, :held])
        weight_grads.append(gw_r)
    dh_from = swap(dh_part[tokens:].astype(BF), 1).astype(F32)
    dgates_from = swap(jnp.concatenate(dgates_away, axis=1), 1)
    out_from = swap(out_part[tokens:].astype(BF), 1).astype(F32)
    for r in range(rounds):
        dgates = lax.dynamic_update_slice_in_dim(
            dgates, dgates_from[:, r * held : (r + 1) * held], (me ^ 1 ^ (2 * r)) * held, 1
        )
    activations = (r1 + RESIDUAL_FACTOR * (out_part[:tokens] + out_from)).astype(BF)

    own_gates = gates[:tokens]
    dlogits = own_gates * (dgates - jnp.sum(own_gates * dgates, axis=-1, keepdims=True))
    dlogits = dlogits.astype(BF)
    grad_router = tn(h2_mine, dlogits)
    dh2 = dh_part[:tokens] + dh_from + nt(dlogits, router_matrix)
    grad_gain_ffn = jnp.sum(dh2 * normed_two, axis=0)
    dr1 = go_mine.astype(F32) + norm_back(dh2 * gain_ffn, normed_two, scale_two)
    dbr = (RESIDUAL_FACTOR * dr1).astype(BF)
    grad_out = tn(dbr, att).astype(BF)
    datt = nn(dbr, out_matrix)

    dq, dkv = attention_back(
        info, queries, kv_all, attended, datt.reshape(seqs, seg_len, width), ml
    )
    dkv = lax.psum_scatter(dkv, "seq", scatter_dimension=0)
    dqkv = unrope(dq, dkv, cosine, sine).reshape(tokens, -1)
    grad_qkv = tn(h1, dqkv).astype(BF)
    dh1 = nt(dqkv, qkv_matrix)
    grad_gain_attn = jnp.sum(dh1 * normed_one, axis=0)
    input_grad = dr1 + norm_back(dh1 * gain_attn, normed_one, scale_one)

    scattered = [lax.psum_scatter(g, "dp", scatter_dimension=0).astype(F32) for g in weight_grads]
    mine = scattered[0]
    for r in range(1, rounds):
        mine = mine + swap(scattered[r].astype(BF), 2 * r).astype(F32)
    hidden = w_down.shape[1]
    grad_gate_up = mine[:, :, : 2 * hidden]
    grad_down = jnp.swapaxes(mine[:, :, 2 * hidden :], 1, 2)
    grad_out = lax.psum_scatter(grad_out, everyone, scatter_dimension=0, tiled=True).astype(F32).T
    grad_qkv = lax.psum_scatter(grad_qkv, everyone, scatter_dimension=0, tiled=True).astype(F32)
    small = jnp.concatenate([grad_gain_attn[:, None], grad_gain_ffn[:, None], grad_router], axis=1)
    small = lax.psum_scatter(small, everyone, scatter_dimension=0, tiled=True)
    return (
        activations.reshape(tokens_in.shape),
        input_grad.reshape(tokens_in.shape),
        small[:, 0],
        grad_qkv,
        grad_out,
        small[:, 1],
        small[:, 2:],
        grad_gate_up,
        grad_down,
    )


def solution(mesh):
    in_specs = (
        P("dp", "seq", None),
        P("dp", "seq", None),
        P("dp"),
        P(("dp", "seq")),
        P(("dp", "seq"), None),
        P(None, ("dp", "seq")),
        P(("dp", "seq")),
        P(("dp", "seq"), None),
        P("seq", "dp", None),
        P("seq", None, "dp"),
        P("dp", "seq", None),
    )
    out_specs = (
        P("dp", "seq", None),
        P("dp", "seq", None),
        P(("dp", "seq")),
        P(("dp", "seq"), None),
        P(None, ("dp", "seq")),
        P(("dp", "seq")),
        P(("dp", "seq"), None),
        P("seq", "dp", None),
        P("seq", None, "dp"),
    )
    return jax.shard_map(body, mesh=mesh, in_specs=in_specs, out_specs=out_specs, check_vma=False)
```
